128 devices in a mesh: leaf: 32 (over y, x, core), sub: 4 (over z).
Axes of the slice: x: 4, y: 4, z: 4, core: 2. Of those that a mesh axis runs over, the one named last changes fastest.
Arguments:
- currents: float32 [262144, 128], P(('leaf', 'sub')), may hold values from -6 to 6
- leaf_basis: float32 [2048, 128, 128], P(('leaf', 'sub')), may hold values from -0.5 to 0.5
- leaf_rank: int32 [2048], P(('leaf', 'sub')), may hold values from 64 to 128
- leaf_transfer: float32 [2048, 128, 128], P(('leaf', 'sub')), may hold values from -0.25 to 0.25
- top_transfer: float32 [32, 4, 128, 128], P('leaf', None, None, 'sub'), may hold values from -0.375 to 0.375
- far_table: float32 [32, 2, 128, 128], replicated, may hold values from -0.125 to 0.125
- send_src: int32 [128, 3, 4, 12], P(('leaf', 'sub')), may hold values from -1 to 15, as said below
- recv_tgt: int32 [128, 3, 4, 12], P(('leaf', 'sub')), may hold values from -1 to 15, as said below
- recv_type: int32 [128, 3, 4, 12], P(('leaf', 'sub')), may hold values from 0 to 31, as said below
- top_coupling: float32 [32, 4, 2, 128, 128], P('leaf', None, None, 'sub'), may hold values from -0.1875 to 0.1875
- top_list: int32 [32, 4], P('leaf'), may hold values from 0 to 31, as said below
- near_blocks: float32 [8192, 2, 128, 128], P(('leaf', 'sub')), may hold values from -0.1875 to 0.1875
- near_tgt: int32 [128, 64], P(('leaf', 'sub')), may hold values from 0 to 15, as said below
- near_src: int32 [128, 64], P(('leaf', 'sub')), may hold values from 0 to 23, as said below
Outputs:
- potential: float32 [262144, 128], P(('leaf', 'sub'))
The draws below stay inside these ranges and needn't reach their ends.
Inputs may be any that keep to these rules, and one draw needn't show every extreme that they name: `send_src`: entry [q, o, s, j] names the leaf of device q (counted from its first leaf) whose coefficients fill slot j of what device q sends to device (q // 4 + o - 1) * 4 + s, or -1 for an empty slot; it is -1 wherever q // 4 + o - 1 lies outside 0 to 31. In every draw some device receives 12 filled slots from every device of its own group and of the two groups beside it. `recv_tgt`: entry [p, o, s, j] is the leaf of device p (counted from its first leaf) on which slot j from device (p // 4 + o - 1) * 4 + s acts; it is -1 exactly where that slot is empty or that device does not exist. `recv_type`: entry [p, o, s, j] selects the matrix of far_table for slot j from device (p // 4 + o - 1) * 4 + s to device p. `top_list`: row g names 4 different groups, none equal to g. `near_tgt`: counted from the device's first leaf. `near_src`: counted from 4 leaves before the device's first leaf; it lies within 4 leaves of the block's target leaf.
All inputs are finite; a program needn't handle non-finite values.
Results may differ from the reference program's by a relative error of at most 0.0003.
Values sent between devices are 32-bit elements; how exact they have to be, the bound alone decides.
No kernel may reach another device: no remote copies, remote signals or barrier semaphores. Data moves between devices by JAX's collectives and lax.ppermute only.
A program may use at most 192 MiB of HBM per device.

```python
import jax
import jax.numpy as jnp
from jax import lax

PANEL = 128
RANK = 128
LEAF_DEV = 16
CAP = 12
NEAR_DEV = 64
HALO_L = 4
NTYPE = 32
K_TOP = 4
DEVS = 128
GROUPS = 32
NLEAVES = 2048
PANELS = 262144
COLS = 128
N_SUB = 4


def far_plan(key):
    base = jax.random.fold_in(key, 17)
    fill_key, roll_key, full_key, source_key, target_key, kind_key = jax.random.split(base, 6)
    fill_share = jax.random.randint(fill_key, (DEVS,), 25, 76)
    roll_value = jax.random.randint(roll_key, (DEVS, 3, N_SUB, CAP), 0, 100)
    full_dest = jax.random.randint(full_key, (), N_SUB, DEVS - N_SUB)
    sender_ids = jnp.arange(DEVS, dtype=jnp.int32)[:, None, None, None]
    offsets = jnp.arange(3, dtype=jnp.int32)[None, :, None, None]
    subs = jnp.arange(N_SUB, dtype=jnp.int32)[None, None, :, None]
    receiver_group = sender_ids // N_SUB + offsets - 1
    receiver_valid = (receiver_group >= 0) & (receiver_group < GROUPS)
    receiver = jnp.clip(receiver_group, 0, GROUPS - 1) * N_SUB + subs
    used_slot = ((roll_value < fill_share[receiver]) | (receiver == full_dest)) & receiver_valid
    source_leaf = jax.random.randint(source_key, (DEVS, 3, N_SUB, CAP), 0, LEAF_DEV)
    target_leaf = jax.random.randint(target_key, (DEVS, 3, N_SUB, CAP), 0, LEAF_DEV)
    kind_ids = jax.random.randint(kind_key, (DEVS, 3, N_SUB, CAP), 0, NTYPE)
    return (used_slot, source_leaf, target_leaf, kind_ids)


def receiver_view(values):
    receivers = jnp.arange(DEVS, dtype=jnp.int32)
    group = receivers // N_SUB
    sub_index = receivers % N_SUB
    offsets = jnp.arange(3, dtype=jnp.int32)
    sender_groups = group[:, None] + offsets[None, :] - 1
    valid = (sender_groups >= 0) & (sender_groups < GROUPS)
    senders = jnp.clip(sender_groups, 0, GROUPS - 1)[:, :, None] * N_SUB + jnp.arange(N_SUB, dtype=jnp.int32)[None, None, :]
    back = jnp.broadcast_to((2 - offsets)[None, :, None], (DEVS, 3, N_SUB))
    subs = jnp.broadcast_to(sub_index[:, None, None], (DEVS, 3, N_SUB))
    return (values[senders, back, subs], jnp.broadcast_to(valid[:, :, None, None], (DEVS, 3, N_SUB, CAP)))


def draw_send_src(key, part):
    used_slot, source_leaf, target_leaf, kind_ids = far_plan(key)
    return jnp.where(used_slot, source_leaf, -1).astype(jnp.int32)


def draw_recv_tgt(key, part):
    used_slot, source_leaf, target_leaf, kind_ids = far_plan(key)
    used_view, valid = receiver_view(used_slot)
    target_view, valid = receiver_view(target_leaf)
    return jnp.where(used_view & valid, target_view, -1).astype(jnp.int32)


def draw_recv_type(key, part):
    used_slot, source_leaf, target_leaf, kind_ids = far_plan(key)
    kind_view, valid = receiver_view(kind_ids)
    return kind_view.astype(jnp.int32)


def near_plan(key):
    base = jax.random.fold_in(key, 29)
    target_key, offset_key = jax.random.split(base, 2)
    target_leaf = jax.random.randint(target_key, (DEVS, NEAR_DEV), 0, LEAF_DEV)
    offsets = jax.random.randint(offset_key, (DEVS, NEAR_DEV), -HALO_L, HALO_L + 1)
    return (target_leaf, target_leaf + HALO_L + offsets)


def draw_near_tgt(key, part):
    target_leaf, source_leaf = near_plan(key)
    return target_leaf.astype(jnp.int32)


def draw_near_src(key, part):
    target_leaf, source_leaf = near_plan(key)
    return source_leaf.astype(jnp.int32)


def draw_top_list(key, part):
    base = jax.random.fold_in(key, 41)
    scores = jax.random.randint(base, (GROUPS, GROUPS), 0, 4096) * GROUPS + jnp.arange(GROUPS, dtype=jnp.int32)[None, :]
    diagonal = jnp.arange(GROUPS, dtype=jnp.int32)[:, None] == jnp.arange(GROUPS, dtype=jnp.int32)[None, :]
    scores = jnp.where(diagonal, 2 ** 30, scores)
    ordering = jnp.argsort(scores, axis=1)
    return ordering[:, :K_TOP].astype(jnp.int32)


def place_ends(array, key, smallest, largest):
    longest = array.shape.index(max(array.shape))
    spots = []
    for shift in (0, 1):
        where = [jax.random.randint(jax.random.fold_in(key, axis), (), 0, length) for axis, length in enumerate(array.shape)]
        where[longest] = (where[longest] + shift) % array.shape[longest]
        spots.append(tuple(where))
    return array.at[spots[0]].set(smallest).at[spots[1]].set(largest)


def shard_levels(stream_key, extent, cuts, smallest, top_value):
    level, own = 1.0, jax.random.fold_in(stream_key, 6)
    for axis_at, parts in cuts:
        steps = jnp.exp(jax.random.uniform(jax.random.fold_in(own, axis_at), (parts,), jnp.float32, smallest / len(cuts), top_value / len(cuts)))
        level = level * jnp.repeat(steps, extent[axis_at] // parts).reshape([-1 if axis == axis_at else 1 for axis in range(len(extent))])
    return level


def scatter_about(own_key, extent, scale, bound, shards=(), kind=jnp.bfloat16):
    factor_of = shard_levels(own_key, extent, shards, -0.22, 0.18) if shards else 1.0
    entries = jax.random.normal(own_key, extent, jnp.float32) * scale * factor_of
    return jnp.minimum(jnp.maximum(entries, -bound), bound).astype(kind)


def setup_inputs(seed: int = 0) -> dict:
    key_of = jax.random.split(jax.random.key(seed), 15)
    return {
        "currents": scatter_about(key_of[0], (PANELS, COLS), 1.0, 6.0, ((0, 128),), jnp.float32),
        "leaf_basis": scatter_about(key_of[1], (NLEAVES, PANEL, RANK), PANEL ** -0.5, 0.5, ((0, 128),), jnp.float32),
        "leaf_rank": place_ends(jax.random.randint(key_of[2], (NLEAVES,), RANK // 2, RANK + 1), jax.random.fold_in(key_of[2], 1), RANK // 2, RANK).astype(jnp.int32),
        "leaf_transfer": scatter_about(key_of[3], (NLEAVES, RANK, RANK), (4 * RANK) ** -0.5, 0.25, ((0, 128),), jnp.float32),
        "top_transfer": scatter_about(key_of[4], (GROUPS, N_SUB, RANK, RANK), (2 * RANK) ** -0.5, 0.375, ((0, 32), (3, 4)), jnp.float32),
        "far_table": scatter_about(key_of[5], (NTYPE, 2, RANK, RANK), (2 * RANK * 3 * N_SUB * CAP // LEAF_DEV) ** -0.5, 0.125, (), jnp.float32),
        "send_src": draw_send_src(jax.random.fold_in(key_of[14], 71), 0),
        "recv_tgt": draw_recv_tgt(jax.random.fold_in(key_of[14], 71), 0),
        "recv_type": draw_recv_type(jax.random.fold_in(key_of[14], 71), 0),
        "top_coupling": scatter_about(key_of[9], (GROUPS, K_TOP, 2, RANK, RANK), (2 * RANK * K_TOP) ** -0.5, 0.1875, ((0, 32), (3, 4)), jnp.float32),
        "top_list": draw_top_list(jax.random.fold_in(key_of[14], 71), 0),
        "near_blocks": scatter_about(key_of[11], (DEVS * NEAR_DEV, 2, PANEL, PANEL), (2 * PANEL * NEAR_DEV // LEAF_DEV) ** -0.5, 0.1875, ((0, 128),), jnp.float32),
        "near_tgt": draw_near_tgt(jax.random.fold_in(key_of[14], 71), 0),
        "near_src": draw_near_src(jax.random.fold_in(key_of[14], 71), 0),
    }


exact_precision = lax.Precision.HIGHEST


def rotate(values):
    middle = values.shape[-1] // 2
    return jnp.concatenate([-values[..., middle:], values[..., :middle]], axis=-1)


def far_device(device, leaf_coef, send_src, recv_tgt, recv_type, far_table):
    group = device // N_SUB
    sub_index = device % N_SUB
    offsets = jnp.arange(3, dtype=jnp.int32)
    sender_groups = group + offsets - 1
    valid = (sender_groups >= 0) & (sender_groups < GROUPS)
    senders = jnp.clip(sender_groups, 0, GROUPS - 1)[:, None] * N_SUB + jnp.arange(N_SUB, dtype=jnp.int32)[None, :]
    back = jnp.broadcast_to((2 - offsets)[:, None], (3, N_SUB))
    sources = send_src[senders, back, sub_index]
    sources = jnp.where(valid[:, None, None], sources, -1)
    leaf_ids = senders[:, :, None] * LEAF_DEV + jnp.maximum(sources, 0)
    present = (sources >= 0).astype(jnp.float32)
    gathered = leaf_coef[leaf_ids] * present[:, :, :, None, None]
    slot_count = 3 * N_SUB * CAP
    gathered = gathered.reshape(slot_count, RANK, gathered.shape[-1])
    kind_ids = lax.dynamic_index_in_dim(recv_type, device, axis=0, keepdims=False).reshape(slot_count)
    targets = lax.dynamic_index_in_dim(recv_tgt, device, axis=0, keepdims=False).reshape(slot_count)
    matrices = far_table[kind_ids]
    operator_product = jnp.einsum("sab,sbc->sac", matrices[:, 0], gathered, precision=exact_precision)
    operator_product = operator_product + jnp.einsum("sab,sbc->sac", matrices[:, 1], rotate(gathered), precision=exact_precision)
    selector_matrix = (targets[:, None] == jnp.arange(LEAF_DEV, dtype=jnp.int32)[None, :]).astype(jnp.float32)
    return jnp.einsum("iv,ibg->vbg", selector_matrix, operator_product, precision=exact_precision)


def near_device(device, leaf_currents, blocks, near_tgt, near_src):
    extended = lax.dynamic_index_in_dim(near_src, device, axis=0, keepdims=False)
    leaf_ids = device * LEAF_DEV + extended - HALO_L
    inside_grid = ((leaf_ids >= 0) & (leaf_ids < NLEAVES)).astype(jnp.float32)
    sources = leaf_currents[jnp.clip(leaf_ids, 0, NLEAVES - 1)] * inside_grid[:, None, None]
    own_blocks = lax.dynamic_index_in_dim(blocks, device, axis=0, keepdims=False)
    operator_product = jnp.einsum("nab,nbc->nac", own_blocks[:, 0], sources, precision=exact_precision)
    operator_product = operator_product + jnp.einsum("nab,nbc->nac", own_blocks[:, 1], rotate(sources), precision=exact_precision)
    targets = lax.dynamic_index_in_dim(near_tgt, device, axis=0, keepdims=False)
    selector_matrix = (targets[:, None] == jnp.arange(LEAF_DEV, dtype=jnp.int32)[None, :]).astype(jnp.float32)
    return jnp.einsum("if,ivo->fvo", selector_matrix, operator_product, precision=exact_precision)


def reference(currents, leaf_basis, leaf_rank, leaf_transfer, top_transfer, far_table, send_src, recv_tgt, recv_type, top_coupling, top_list, near_blocks, near_tgt, near_src):
    columns = currents.shape[1]
    rank_mask = (jnp.arange(RANK, dtype=jnp.int32)[None, :] < leaf_rank[:, None]).astype(jnp.float32)
    masked_basis = leaf_basis * rank_mask[:, None, :]
    leaf_currents = currents.reshape(NLEAVES, PANEL, columns)
    leaf_coef = jnp.einsum("lpr,lpc->lrc", masked_basis, leaf_currents, precision=exact_precision)
    lifted = jnp.einsum("lab,lac->lbc", leaf_transfer, leaf_coef, precision=exact_precision)
    mid_coef = lifted.reshape(DEVS, LEAF_DEV, RANK, columns).sum(axis=1)
    grouped = mid_coef.reshape(GROUPS, N_SUB, RANK, columns)
    top_coef = jnp.einsum("gsab,gsac->gbc", top_transfer, grouped, precision=exact_precision)
    partners = top_coef[top_list]
    top_field = jnp.einsum("gkab,gkbc->gac", top_coupling[:, :, 0], partners, precision=exact_precision)
    top_field = top_field + jnp.einsum("gkab,gkbc->gac", top_coupling[:, :, 1], rotate(partners), precision=exact_precision)
    mid_field = jnp.einsum("gsab,gbc->gsac", top_transfer, top_field, precision=exact_precision).reshape(DEVS, RANK, columns)
    down_field = jnp.einsum("lab,lbc->lac", leaf_transfer, jnp.repeat(mid_field, LEAF_DEV, axis=0), precision=exact_precision)
    far_field = lax.map(lambda device: far_device(device, leaf_coef, send_src, recv_tgt, recv_type, far_table), jnp.arange(DEVS, dtype=jnp.int32))
    leaf_field = far_field.reshape(NLEAVES, RANK, columns) + down_field
    far_part = jnp.einsum("lpr,lrc->lpc", masked_basis, leaf_field, precision=exact_precision)
    blocks = near_blocks.reshape(DEVS, NEAR_DEV, 2, PANEL, PANEL)
    near_field_share = lax.map(lambda device: near_device(device, leaf_currents, blocks, near_tgt, near_src), jnp.arange(DEVS, dtype=jnp.int32))
    near_field_share = near_field_share.reshape(NLEAVES, PANEL, columns)
    return (far_part + near_field_share).reshape(PANELS, columns)
```

```python
import functools

import jax
import jax.numpy as jnp
from jax import lax
from jax.experimental import pallas as pl
from jax.experimental.pallas import tpu as pltpu
from jax.sharding import PartitionSpec as P

HALO_L = 4
F32 = jnp.float32
BF16 = jnp.bfloat16
N = 128
LEAVES = 16
HALF = 8
SUBS = 4
CAP = 12
ROWS_A = HALF * N + 8


def moved(value, axis, by):
    length = lax.axis_size(axis)
    return lax.ppermute(value, axis, [(i, (i + by) % length) for i in range(length)])


def shifted(value, axis, by):
    length = lax.axis_size(axis)
    return lax.ppermute(value, axis, [(i, i + by) for i in range(length) if 0 <= i + by < length])


def split(x):
    hi = x.astype(BF16)
    lo = (x - hi.astype(F32)).astype(BF16)
    return hi, lo


def dot(a, b, ca=1, cb=0):
    return lax.dot_general(a, b, (((ca,), (cb,)), ((), ())), preferred_element_type=F32)


def dot3(a, b, ca=1, cb=0):
    ah, al = split(a)
    bh, bl = split(b)
    return dot(ah, bh, ca, cb) + (dot(ah, bl, ca, cb) + dot(al, bh, ca, cb))


def rotate(x):
    lanes = lax.broadcasted_iota(jnp.int32, x.shape, 1)
    turned = pltpu.roll(x, x.shape[1] // 2, axis=1)
    return jnp.where(lanes < x.shape[1] // 2, -turned, turned)


def put_source(dst, x):
    hi, lo = split(x)
    dst[0:N, 0:N] = hi
    dst[0:N, N : 2 * N] = lo
    hi, lo = split(rotate(x))
    dst[N : 2 * N, 0:N] = hi
    dst[N : 2 * N, N : 2 * N] = lo


VMEM = pl.BlockSpec(memory_space=pltpu.VMEM)
SMEM = pl.BlockSpec(memory_space=pltpu.SMEM)
ANY = pl.BlockSpec(memory_space=pl.ANY)


def sds(shape, dtype=F32):
    return jax.ShapeDtypeStruct(shape, dtype)


def cost(flops):
    return pl.CostEstimate(flops=int(flops), bytes_accessed=0, transcendentals=0)


def coef_kernel(rank, rider, cur, basis, transfer, a_out, b_out, mid_out, cur_v, bas_v, tra_v, sems):
    chunk = 4
    steps = LEAVES // chunk

    def copies(c):
        rows = pl.ds(c * chunk * N, chunk * N)
        ids = pl.ds(c * chunk, chunk)
        return (
            pltpu.make_async_copy(cur.at[rows], cur_v.at[rows], sems.at[0, c]),
            pltpu.make_async_copy(basis.at[ids], bas_v.at[ids], sems.at[1, c]),
            pltpu.make_async_copy(transfer.at[ids], tra_v.at[ids], sems.at[2, c]),
        )

    for c in range(steps):
        for copy in copies(c):
            copy.start()
    a_out[HALF * N : ROWS_A, :] = rider[...]
    rows_of = lax.broadcasted_iota(jnp.int32, (N, N), 0)
    mid = jnp.zeros((N, N), F32)
    for c in range(steps):
        for copy in copies(c):
            copy.wait()
        for i in range(c * chunk, (c + 1) * chunk):
            coef = dot3(bas_v[i], cur_v[i * N : (i + 1) * N, :], 0, 0)
            coef = jnp.where(rows_of < rank[i], coef, 0.0)
            if i < HALF:
                a_out[i * N : (i + 1) * N, :] = coef
            else:
                b_out[(i - HALF) * N : (i - HALF + 1) * N, :] = coef
            mid = mid + dot3(tra_v[i], coef, 0, 0)
    mid_out[...] = mid


def leaf_coefficients(rank, rider, currents, basis, transfer):
    return pl.pallas_call(
        coef_kernel,
        in_specs=[SMEM, VMEM, ANY, ANY, ANY],
        out_specs=[VMEM, VMEM, VMEM],
        out_shape=[sds((ROWS_A, N)), sds((HALF * N, N)), sds((N, N))],
        scratch_shapes=[
            pltpu.VMEM((LEAVES * N, N), F32),
            pltpu.VMEM((LEAVES, N, N), F32),
            pltpu.VMEM((LEAVES, N, N), F32),
            pltpu.SemaphoreType.DMA((3, 4)),
        ],
        cost_estimate=cost(4e6 * 32 * 4),
        name="leaf_coefficients",
    )(rank, rider, currents, basis, transfer)


def table_kernel(tab, out):
    for t in range(tab.shape[0]):
        for part in range(2):
            hi, lo = split(tab[t, part])
            out[t, 0:N, part * N : (part + 1) * N] = hi
            out[t, N : 2 * N, part * N : (part + 1) * N] = lo


def split_table(table):
    count = table.shape[0]
    step = 8
    return pl.pallas_call(
        table_kernel,
        grid=(count // step,),
        in_specs=[pl.BlockSpec((step, 2, N, N), lambda i: (i, 0, 0, 0))],
        out_specs=pl.BlockSpec((step, 2 * N, 2 * N), lambda i: (i, 0, 0)),
        out_shape=sds((count, 2 * N, 2 * N), BF16),
        cost_estimate=cost(4e6 * 60),
        name="split_table",
    )(table)


def product(matrix, source):
    first = dot(matrix[0:N, :], source)
    second = dot(matrix[N : 2 * N, :], source[:, 0:N])
    return first[:, 0:N] + (first[:, N : 2 * N] + second)


def near_kernel(tgt, src, below, cur, above, blocks, out, xr):
    step = pl.program_id(0)
    per = blocks.shape[0]

    @pl.when(step == 0)
    def prepare():
        out[...] = jnp.zeros_like(out)
        for i in range(HALO_L):
            put_source(xr.at[i], below[i * N : (i + 1) * N, :])
            put_source(xr.at[HALO_L + LEAVES + i], above[i * N : (i + 1) * N, :])

        def one(i, carry):
            start = pl.multiple_of(i * N, N)
            put_source(xr.at[HALO_L + i], cur[pl.ds(start, N), :])
            return carry

        lax.fori_loop(0, LEAVES, one, 0, unroll=2)

    for i in range(per):
        h0, l0 = split(blocks[i, 0])
        h1, l1 = split(blocks[i, 1])
        source = xr[src[0, step * per + i]]
        first = dot(jnp.concatenate([h0, h1], axis=1), source)
        second = dot(jnp.concatenate([l0, l1], axis=1), source[:, 0:N])
        value = first[:, 0:N] + (first[:, N : 2 * N] + second)
        to = tgt[0, step * per + i]
        out[to] = out[to] + value


def near_field(tgt, src, below, currents, above, blocks):
    count = blocks.shape[0]
    per = 8
    whole = lambda *dims: pl.BlockSpec(dims, lambda i: (0,) * len(dims))
    return pl.pallas_call(
        near_kernel,
        grid=(count // per,),
        in_specs=[
            SMEM,
            SMEM,
            whole(HALO_L * N, N),
            whole(LEAVES * N, N),
            whole(HALO_L * N, N),
            pl.BlockSpec((per, 2, N, N), lambda i: (i, 0, 0, 0)),
        ],
        out_specs=whole(LEAVES, N, N),
        out_shape=sds((LEAVES, N, N)),
        scratch_shapes=[pltpu.VMEM((LEAVES + 2 * HALO_L, 2 * N, 2 * N), BF16)],
        cost_estimate=cost(4e6 * 64 * 2 * 6),
        name="near_field",
    )(tgt, src, below, currents, above, blocks)


UNROLL = 4


def far_kernel(turns, dests, has_base, *refs):
    refs = list(refs)
    meta = refs.pop(0)
    own_tab = refs.pop(0)
    up_tab = refs.pop(0)
    dn_tab = refs.pop(0)
    own_src = refs.pop(0)
    table = refs.pop(0)
    pairs = [(refs.pop(0), refs.pop(0)) for _ in turns]
    bases = [refs.pop(0) for _ in dests] if has_base else None
    outs = [refs.pop(0) for _ in dests]
    xr, acc, ints_v, ints_s, lists, sems = refs

    s = meta[0]
    copies = []
    for n, turn in enumerate(turns):
        if turn:
            a, b = pairs[n]
            ints_v[n] = a[HALF * N : ROWS_A, :].astype(jnp.int32)
            copy = pltpu.make_async_copy(ints_v.at[n], ints_s.at[n], sems.at[n])
            copy.start()
            copies.append(copy)

    for n, turn in enumerate(turns):
        a, b = pairs[n]

        def one(i, carry, a=a, b=b, n=n):
            start = pl.multiple_of(i * N, N)
            put_source(xr.at[n * LEAVES + i], a[pl.ds(start, N), :])
            put_source(xr.at[n * LEAVES + HALF + i], b[pl.ds(start, N), :])
            return carry

        lax.fori_loop(0, HALF, one, 0)
    for m in range(len(dests)):
        if has_base:
            acc[m * LEAVES : (m + 1) * LEAVES] = bases[m][...]
        else:
            acc[m * LEAVES : (m + 1) * LEAVES] = jnp.zeros((LEAVES, N, N), F32)
    for copy in copies:
        copy.wait()

    count = jnp.int32(0)
    for m, dest in enumerate(dests):
        tab, sender_o, recv_o = {
            "own": (own_tab, 1, 1),
            "up": (up_tab, 2, 0),
            "down": (dn_tab, 0, 2),
        }[dest]
        for n, turn in enumerate(turns):
            q = lax.rem(s + turn, SUBS)

            def scan(j, count, n=n, m=m, turn=turn, q=q, tab=tab, sender_o=sender_o, recv_o=recv_o):
                if turn:
                    leaf = ints_s[n, sender_o, s * CAP + j]
                else:
                    leaf = own_src[sender_o, s * CAP + j]
                lists[0, count] = leaf + n * LEAVES
                lists[1, count] = tab[3 + recv_o, q * CAP + j]
                lists[2, count] = tab[recv_o, q * CAP + j] + m * LEAVES
                return count + (leaf >= 0).astype(jnp.int32)

            count = lax.fori_loop(0, CAP, scan, count)
    for i in range(UNROLL):
        lists[0, count + i] = 0
        lists[1, count + i] = 0
        lists[2, count + i] = len(dests) * LEAVES

    def body(g, carry):
        for i in range(UNROLL):
            at = g * UNROLL + i
            value = product(table[lists[1, at]], xr[lists[0, at]])
            to = lists[2, at]
            acc[to] = acc[to] + value
        return carry

    lax.fori_loop(0, (count + UNROLL - 1) // UNROLL, body, 0)
    for m in range(len(dests)):
        outs[m][...] = acc[m * LEAVES : (m + 1) * LEAVES]


def far_field(turns, dests, meta, own_tab, up_tab, dn_tab, own_src, table, pairs, bases, name):
    operands = [meta, own_tab, up_tab, dn_tab, own_src, table]
    specs = [SMEM] * 5 + [VMEM]
    for a, b in pairs:
        operands += [a, b]
        specs += [VMEM, VMEM]
    if bases is not None:
        operands += list(bases)
        specs += [VMEM] * len(bases)
    slots = len(turns) * len(dests) * CAP
    return pl.pallas_call(
        functools.partial(far_kernel, turns, dests, bases is not None),
        in_specs=specs,
        out_specs=[VMEM] * len(dests),
        out_shape=[sds((LEAVES, N, N))] * len(dests),
        scratch_shapes=[
            pltpu.VMEM((len(turns) * LEAVES, 2 * N, 2 * N), BF16),
            pltpu.VMEM((len(dests) * LEAVES + 1, N, N), F32),
            pltpu.VMEM((len(turns), 8, N), jnp.int32),
            pltpu.SMEM((len(turns), 8, N), jnp.int32),
            pltpu.SMEM((3, slots + UNROLL), jnp.int32),
            pltpu.SemaphoreType.DMA((len(turns),)),
        ],
        cost_estimate=cost(4e6 * slots * 2 * 6),
        name=name,
    )(*operands)


def share_kernel(meta, transfer, m0, m1, m2, m3, out):
    s = meta[0]
    total = jnp.zeros(out.shape, F32)
    for turn, m in enumerate((m0, m1, m2, m3)):
        total = total + dot3(transfer[lax.rem(s + turn, SUBS)], m[...], 0, 0)
    out[...] = total


def top_share(meta, transfer, mids):
    return pl.pallas_call(
        share_kernel,
        in_specs=[SMEM] + [VMEM] * 5,
        out_specs=VMEM,
        out_shape=sds((transfer.shape[2], N)),
        cost_estimate=cost(4e6 * 6),
        name="top_share",
    )(meta, transfer, *mids)


def select_kernel(meta, chosen, b0, b1, b2, b3, out):
    g = meta[1]
    for k in range(out.shape[0]):
        p = chosen[0, k]
        dy = ((p >> 3) - (g >> 3)) & 3
        dx = ((p >> 1) - (g >> 1)) & 3
        dc = (p ^ g) & 1
        for turn, b in enumerate((b0, b1, b2, b3)):

            @pl.when(dy == turn)
            def take(b=b, k=k):
                out[k] = b[dx * 2 + dc]


def select_partners(meta, chosen, blocks):
    return pl.pallas_call(
        select_kernel,
        in_specs=[SMEM, SMEM] + [VMEM] * 4,
        out_specs=VMEM,
        out_shape=sds((chosen.shape[1],) + blocks[0].shape[1:]),
        cost_estimate=cost(4e6 * 3),
        name="select_partners",
    )(meta, chosen, *blocks)


def group_kernel(meta, coupling, transfer, p0, p1, p2, p3, o0, o1, o2, o3, full):
    s = meta[0]
    width = p0.shape[1]
    for turn, p in enumerate((p0, p1, p2, p3)):
        start = pl.multiple_of(lax.rem(s + turn, SUBS) * width, width)
        full[:, pl.ds(start, width), :] = p[...]
    total = jnp.zeros((width, N), F32)
    for k in range(coupling.shape[0]):
        total = total + dot3(coupling[k, 0], full[k])
        total = total + dot3(coupling[k, 1], rotate(full[k]))
    for turn, o in enumerate((o0, o1, o2, o3)):
        o[...] = dot3(transfer[lax.rem(s + turn, SUBS)], total)


def group_fields(meta, coupling, transfer, parts):
    return pl.pallas_call(
        group_kernel,
        in_specs=[SMEM] + [VMEM] * 6,
        out_specs=[VMEM] * 4,
        out_shape=[sds((N, N))] * 4,
        scratch_shapes=[pltpu.VMEM((coupling.shape[0], N, N), F32)],
        cost_estimate=cost(4e6 * 20),
        name="group_fields",
    )(meta, coupling, transfer, *parts)


def final_kernel(rank, own, up, dn, m0, m1, m2, m3, transfer, basis, near, out):
    per = basis.shape[0]
    step = pl.program_id(0)
    mh, ml = split(m0[...] + m1[...] + (m2[...] + m3[...]))
    rows_of = lax.broadcasted_iota(jnp.int32, (N, N), 0)
    for i in range(per):
        th, tl = split(transfer[i])
        field = dot(th, mh) + (dot(th, ml) + dot(tl, mh))
        field = own[i] + (up[i] + dn[i]) + field
        field = jnp.where(rows_of < rank[step * per + i], field, 0.0)
        out[i * N : (i + 1) * N, :] = dot3(basis[i], field) + near[i]


def potentials(rank, own, up, dn, mids, transfer, basis, near):
    per = 4
    leaf = pl.BlockSpec((per, N, N), lambda i: (i, 0, 0))
    return pl.pallas_call(
        final_kernel,
        grid=(LEAVES // per,),
        in_specs=[SMEM, leaf, leaf, leaf] + [pl.BlockSpec((N, N), lambda i: (0, 0))] * 4 + [leaf, leaf, leaf],
        out_specs=pl.BlockSpec((per * N, N), lambda i: (i, 0)),
        out_shape=sds((LEAVES * N, N)),
        cost_estimate=cost(4e6 * 32 * 6),
        name="potentials",
    )(rank, own, up, dn, *mids, transfer, basis, near)


def per_device(
    currents,
    leaf_basis,
    leaf_rank,
    leaf_transfer,
    top_transfer,
    far_table,
    send_src,
    recv_tgt,
    recv_type,
    top_coupling,
    top_list,
    near_blocks,
    near_tgt,
    near_src,
):
    meta = jnp.stack([lax.axis_index("sub"), lax.axis_index("leaf")]).astype(jnp.int32)
    sends = send_src[0].reshape(3, SUBS * CAP)
    rider = jnp.pad(sends.astype(F32), ((0, 5), (0, N - SUBS * CAP)))
    tables = jnp.concatenate(
        [recv_tgt[0].reshape(3, SUBS * CAP), recv_type[0].reshape(3, SUBS * CAP)], axis=0
    )
    rim = HALO_L * N
    below = shifted(currents[currents.shape[0] - rim :], ("leaf", "sub"), 1)
    above = shifted(currents[:rim], ("leaf", "sub"), -1)
    up_tab = shifted(tables, "leaf", -1)
    dn_tab = shifted(tables, "leaf", 1)

    coef_a, coef_b, mid = leaf_coefficients(leaf_rank, rider, currents, leaf_basis, leaf_transfer)

    mids = [mid, moved(mid, "sub", -1), moved(mid, "sub", 2), moved(mid, "sub", 1)]
    a_from = {3: moved(coef_a, "sub", 1), 1: moved(coef_a, "sub", -1)}
    b_from = {1: moved(coef_b, "sub", -1), 3: moved(coef_b, "sub", 1)}
    a_from[2] = moved(a_from[3], "sub", 1)
    b_from[2] = moved(b_from[1], "sub", -1)

    table = split_table(far_table)
    near = near_field(near_tgt, near_src, below, currents, above, near_blocks)

    share = top_share(meta, top_transfer[0], mids)
    groups = lax.axis_size("leaf")

    def turned(value, where):
        return lax.ppermute(value, "leaf", [(where(i), i) for i in range(groups)])

    def at(dy, dx, dc):
        return lambda i: ((((i >> 3) + dy) & 3) << 3) | ((((i >> 1) + dx) & 3) << 1) | ((i ^ dc) & 1)

    pair = jnp.stack([share, turned(share, at(0, 0, 1))])
    line = jnp.concatenate([pair] + [turned(pair, at(0, d, 0)) for d in (1, 2, 3)], axis=0)
    planes = [line] + [turned(line, at(d, 0, 0)) for d in (1, 2, 3)]
    partners = select_partners(meta, top_list, planes)
    parts = [partners, moved(partners, "sub", -1), moved(partners, "sub", 2), moved(partners, "sub", 1)]
    fields = group_fields(meta, top_coupling[0], top_transfer[0], parts)
    mid_parts = [fields[0], moved(fields[1], "sub", 1), moved(fields[2], "sub", 2), moved(fields[3], "sub", -1)]

    far = functools.partial(far_field, meta=meta, own_tab=tables, up_tab=up_tab, dn_tab=dn_tab, own_src=sends, table=table)
    own, up, dn = far(
        (0, 1, 3),
        ("own", "up", "down"),
        pairs=[(coef_a, coef_b), (a_from[1], b_from[1]), (a_from[3], b_from[3])],
        bases=None,
        name="far_first",
    )
    last = [(a_from[2], b_from[2])]
    up, dn = far((2,), ("up", "down"), pairs=last, bases=[up, dn], name="far_out")
    from_below = shifted(up, "leaf", 1)
    from_above = shifted(dn, "leaf", -1)
    (own,) = far((2,), ("own",), pairs=last, bases=[own], name="far_own")
    return potentials(leaf_rank, own, from_below, from_above, mid_parts, leaf_transfer, leaf_basis, near)


def solution(mesh):
    placed = (
        P(("leaf", "sub"), None),
        P(("leaf", "sub"), None, None),
        P(("leaf", "sub")),
        P(("leaf", "sub"), None, None),
        P("leaf", None, None, "sub"),
        P(),
        P(("leaf", "sub"), None, None, None),
        P(("leaf", "sub"), None, None, None),
        P(("leaf", "sub"), None, None, None),
        P("leaf", None, None, "sub", None),
        P("leaf", None),
        P(("leaf", "sub"), None, None, None),
        P(("leaf", "sub"), None),
        P(("leaf", "sub"), None),
    )
    return jax.shard_map(
        per_device, mesh=mesh, in_specs=placed, out_specs=P(("leaf", "sub"), None), check_vma=False
    )
```
